32 devices in a mesh: groups: 2 (over x), seq: 16 (over z, y, core).
Axes of the slice: x: 2, y: 2, z: 4, core: 2. Of those that a mesh axis runs over, the one named last changes fastest.
Arguments:
- self_query: bfloat16 [16, 8192], P('groups'), parts along dimension 0, may hold values from -128 to 128
- new_key: bfloat16 [16, 8192], P('groups'), parts along dimension 0, may hold values from -6 to 6
- new_value: bfloat16 [16, 8192], P('groups'), parts along dimension 0, may hold values from -12 to 12
- cache_keys: bfloat16 [16, 1024, 8192], P('groups', 'seq'), parts along dimension 0, may hold values from -8 to 8
- cache_values: bfloat16 [16, 1024, 8192], P('groups', 'seq'), parts along dimension 0, may hold values from -12 to 12
- lengths: int32 [16], P('groups'), parts along dimension 0, may hold values from 128 to 1024
- db_keys: bfloat16 [32, 128, 8192], P(('groups', 'seq')), parts along dimension 0, may hold values from -8 to 8
- db_values: bfloat16 [32, 128, 8192], P(('groups', 'seq')), parts along dimension 0, may hold values from -12 to 12
- cross_query: bfloat16 [16, 8192], P('groups'), parts along dimension 0, may hold values from -128 to 128
- neighbour_ids: int32 [16, 2], P('groups'), parts along dimension 0, may hold values from 0 to 15
Outputs:
- self_out: bfloat16 [16, 8192], P('groups', 'seq'), parts along dimension 0
- cross_out: bfloat16 [16, 8192], P('groups', 'seq'), parts along dimension 0
The draws below stay inside these ranges and needn't reach their ends.
There are 2 independent parts, one for each index of `groups`. The reference program is written for one: setup_inputs(seed, part) draws one part's arguments, and reference() takes and returns one part's arrays. A program takes and returns all parts, laid end to end along the dimension named above; each array names one. Nothing has to cross between parts.
Inputs may be any that keep to these rules, and one draw needn't show every extreme that they name: `neighbour_ids`: the 2 ids of a row may repeat.
All inputs are finite; a program needn't handle non-finite values.
Results may differ from the reference program's by a relative error of at most 0.022.
Values may be sent and summed in bfloat16 or wider, within the bound.
A program may use at most 64 MiB of HBM per device.

```python
import jax
import jax.numpy as jnp
from jax import lax

H = 64
DH = 128
HD = 8192
ROWS = 8
L = 1024
NBR = 2
NTOK = 128
NDB = 16


def draw_cache_keys(key, part):
    keys = jax.random.normal(jax.random.fold_in(key, 11), (ROWS, L, HD), jnp.float32)
    return keys.astype(jnp.bfloat16)


def draw_self_query(key, part):
    query = 1.5 * jax.random.normal(jax.random.fold_in(key, 12), (ROWS, HD), jnp.float32)
    return query.astype(jnp.bfloat16)


def draw_db_keys(key, part):
    keys = jax.random.normal(jax.random.fold_in(key, 13), (NDB, NTOK, HD), jnp.float32)
    return keys.astype(jnp.bfloat16)


def draw_cross_query(key, part):
    query = 1.5 * jax.random.normal(jax.random.fold_in(key, 14), (ROWS, HD), jnp.float32)
    return query.astype(jnp.bfloat16)


def place_ends(result, own_key, smallest, largest):
    longest = result.shape.index(max(result.shape))
    spots = []
    for shift in (0, 1):
        where = [jax.random.randint(jax.random.fold_in(own_key, axis), (), 0, length) for axis, length in enumerate(result.shape)]
        where[longest] = (where[longest] + shift) % result.shape[longest]
        spots.append(tuple(where))
    return result.at[spots[0]].set(smallest).at[spots[1]].set(largest)


def block_scale(stream_key, extent, pieces, smallest, top_value):
    def one(position, blocks):
        draws = jax.random.uniform(jax.random.fold_in(jax.random.fold_in(stream_key, 6), position), (blocks,), jnp.float32, smallest / len(pieces), top_value / len(pieces))
        return jnp.repeat(jnp.exp(draws), extent[position] // blocks).reshape((-1,) + (1,) * (len(extent) - position - 1))

    level = one(*pieces[0])
    for cut in pieces[1:]:
        level = level * one(*cut)
    return level


def normal_values(key, dims, width, most, shards=(), held_as=jnp.bfloat16):
    level = block_scale(key, dims, shards, -0.22, 0.18) if shards else 1.0
    array = jax.random.normal(key, dims, jnp.float32) * width * level
    return jnp.minimum(jnp.maximum(array, -most), most).astype(held_as)


def setup_inputs(seed: int = 0, part: int = 0) -> dict:
    splits = jax.random.split(jax.random.key(seed), 11)
    part_keys = jax.random.split(jax.random.fold_in(splits[10], part), 11)
    return {
        "self_query": draw_self_query(jax.random.fold_in(jax.random.fold_in(splits[10], part), 71), part),
        "new_key": normal_values(part_keys[1], (ROWS, HD), 1.0, 6.0),
        "new_value": normal_values(part_keys[2], (ROWS, HD), 3.0, 12.0),
        "cache_keys": draw_cache_keys(jax.random.fold_in(jax.random.fold_in(splits[10], part), 71), part),
        "cache_values": normal_values(part_keys[4], (ROWS, L, HD), 3.0, 12.0, ((1, 16),)),
        "lengths": place_ends(jax.random.randint(part_keys[5], (ROWS,), max(16, L // 8), L + 1), jax.random.fold_in(part_keys[5], 1), max(16, L // 8), L).astype(jnp.int32),
        "db_keys": draw_db_keys(jax.random.fold_in(jax.random.fold_in(splits[10], part), 71), part),
        "db_values": normal_values(part_keys[7], (NDB, NTOK, HD), 3.0, 12.0, ((0, 16),)),
        "cross_query": draw_cross_query(jax.random.fold_in(jax.random.fold_in(splits[10], part), 71), part),
        "neighbour_ids": place_ends(jax.random.randint(part_keys[9], (ROWS, NBR), 0, NDB), jax.random.fold_in(part_keys[9], 1), 0, NDB - 1).astype(jnp.int32),
    }


NEG = -1e30


def self_row(args):
    query, keys, values, key_new, value_new, length = args
    scale = DH ** -0.5
    q = query.astype(jnp.float32).reshape(H, DH)
    k = keys.astype(jnp.float32).reshape(L, H, DH)
    s = jnp.einsum('hd,phd->hp', q, k) * scale
    live = jnp.arange(L, dtype=jnp.int32)[None, :] < length
    s = jnp.where(live, s, NEG)
    s_own = jnp.sum(q * key_new.astype(jnp.float32).reshape(H, DH), axis=1) * scale
    peak = jnp.maximum(jnp.max(s, axis=1), s_own)
    e = jnp.where(live, jnp.exp(s - peak[:, None]), 0.0)
    e_own = jnp.exp(s_own - peak)
    den = jnp.sum(e, axis=1) + e_own
    w = e.astype(jnp.bfloat16).astype(jnp.float32)
    w_own = e_own.astype(jnp.bfloat16).astype(jnp.float32)
    v = values.astype(jnp.float32).reshape(L, H, DH)
    num = jnp.einsum('hp,phd->hd', w, v) + w_own[:, None] * value_new.astype(jnp.float32).reshape(H, DH)
    return (num / den[:, None]).reshape(HD).astype(jnp.bfloat16)


def cross_row(args):
    query, ids, db_keys, db_values = args
    scale = DH ** -0.5
    q = query.astype(jnp.float32).reshape(H, DH)
    k = jnp.take(db_keys, ids, axis=0).astype(jnp.float32).reshape(NBR * NTOK, H, DH)
    v = jnp.take(db_values, ids, axis=0).astype(jnp.float32).reshape(NBR * NTOK, H, DH)
    s = jnp.einsum('hd,thd->ht', q, k) * scale
    peak = jnp.max(s, axis=1)
    e = jnp.exp(s - peak[:, None])
    den = jnp.sum(e, axis=1)
    w = e.astype(jnp.bfloat16).astype(jnp.float32)
    num = jnp.einsum('ht,thd->hd', w, v)
    return (num / den[:, None]).reshape(HD).astype(jnp.bfloat16)


def reference(self_query, new_key, new_value, cache_keys, cache_values, lengths, db_keys, db_values, cross_query, neighbour_ids):
    self_out = lax.map(self_row, (self_query, cache_keys, cache_values, new_key, new_value, lengths.astype(jnp.int32)))
    cross_out = lax.map(lambda a: cross_row((a[0], a[1], db_keys, db_values)), (cross_query, neighbour_ids.astype(jnp.int32)))
    return self_out, cross_out
```

```python
import functools

import jax
import jax.numpy as jnp
from jax import lax
from jax.experimental import pallas as pl
from jax.experimental.pallas import tpu as pltpu
from jax.sharding import PartitionSpec as P

DH = 128
NEG = -1e30
FLOOR = -1e29
MESH = pl.DeviceIdType.MESH


def mirrored(index, flip, count):
    if count & (count - 1):
        return lax.rem(index + flip, count)
    result, bit = 0, 1
    while bit < count:
        digit = lax.rem(index // bit, 2)
        result = result + bit * (1 - digit if flip & bit else digit)
        bit *= 2
    return result


def kernel(
    parts,
    gather,
    loads,
    ahead,
    plan,
    lengths_in,
    ids_in,
    self_query,
    new_key,
    new_value,
    cache_keys,
    cache_values,
    db_keys,
    db_values,
    cross_query,
    out,
    lengths,
    ids,
    keys,
    values,
    dkeys,
    dvalues,
    squery,
    cquery,
    nkey,
    nvalue,
    marks,
    bias,
    cbias,
    ccounts,
    scores,
    cscores,
    outbox,
    sidebox,
    merged,
    inbox,
    stats,
    stream_sem,
    small_sem,
    send_sem,
    recv_sem,
    side_send,
    side_recv,
):
    me = lax.axis_index("seq")
    rows, positions, width = cache_keys.shape
    entries, tokens, _ = db_keys.shape
    extent = entries * tokens
    span = width // parts
    heads = span // DH
    pairs = heads // 2
    pair_rows = 2 * rows
    groups = parts // gather
    members = gather // 2
    chips = parts // 2
    total = gather * heads * rows
    copies = DH // positions
    chunks = rows // copies

    core = lax.rem(me, 2)
    chip = me // 2
    partner = chip * 2 + 1 - core
    member = lax.rem(chip, members)
    group = chip // members

    def group_at(turn):
        return mirrored(group, groups - 1 - turn, groups)

    def member_at(place):
        return lax.rem(member + 1 + place, members)

    def peer(turn, place):
        return (group_at(turn) * members + member_at(place)) * 2 + core

    def lanes_of(device):
        return pl.ds(pl.multiple_of(device * span, span), span)

    def owner(turn, slot):
        return peer(turn, slot // 2) - core + (core if slot % 2 else 1 - core)

    def stream(kind, turn, slots):
        source, dest = (
            (cache_keys, keys),
            (cache_values, values),
            (db_keys, dkeys),
            (db_values, dvalues),
        )[kind]
        return [
            pltpu.make_async_copy(
                source.at[:, :, lanes_of(owner(turn, s))],
                dest.at[turn, s],
                stream_sem.at[kind, turn, s],
            )
            for s in slots
        ]

    def handover(turn, place):
        step = turn * members + place
        return pltpu.make_async_remote_copy(
            src_ref=outbox.at[turn, 2 * place],
            dst_ref=sidebox.at[step],
            send_sem=side_send.at[step],
            recv_sem=side_recv.at[step],
            device_id={"seq": partner},
            device_id_type=MESH,
        )

    def message(turn, place):
        step = turn * members + place
        return pltpu.make_async_remote_copy(
            src_ref=merged.at[step],
            dst_ref=inbox.at[step],
            send_sem=send_sem.at[step],
            recv_sem=recv_sem.at[step],
            device_id={"seq": peer(turn, place)},
            device_id_type=MESH,
        )

    steps = [(turn, place) for turn in range(groups) for place in range(members)]

    own = lanes_of(me)
    small = [
        pltpu.make_async_copy(self_query, squery, small_sem.at[0]),
        pltpu.make_async_copy(cross_query, cquery, small_sem.at[1]),
        pltpu.make_async_copy(new_key.at[:, own], nkey, small_sem.at[2]),
        pltpu.make_async_copy(new_value.at[:, own], nvalue, small_sem.at[3]),
    ]
    scalars = [
        pltpu.make_async_copy(lengths_in, lengths, small_sem.at[4]),
        pltpu.make_async_copy(ids_in, ids, small_sem.at[5]),
    ]
    everything = range(gather)
    queue = []
    for name in loads:
        turn = int(name[1])
        slots = everything if len(name) == 2 else (2 * int(name[2]), 2 * int(name[2]) + 1)
        for kind in (0, 2) if name[0] == "K" else (1, 3):
            queue.append((kind, turn, slots))

    def launch(count):
        for _ in range(count):
            if queue:
                for copy in stream(*queue.pop(0)):
                    copy.start()

    small[0].start()
    launch(1)
    small[1].start()
    launch(1)
    barrier = pltpu.get_barrier_semaphore()
    for turn, place in steps[:-1]:
        pl.semaphore_signal(
            barrier, inc=1, device_id={"seq": peer(turn, place)}, device_id_type=MESH
        )
    pl.semaphore_signal(barrier, inc=1, device_id={"seq": partner}, device_id_type=MESH)

    for copy in scalars:
        copy.start()
    launch(ahead)
    small[2].start()
    small[3].start()
    tag = lax.broadcasted_iota(jnp.int32, (pair_rows, DH), 1)
    zero = jnp.zeros((rows, DH), jnp.float32)

    def prepare():
        line = lax.rem(lax.broadcasted_iota(jnp.int32, (pair_rows, DH), 0), rows)
        for j in range(chunks):
            mark = jnp.where(line == j * copies + tag // positions, 1.0, 0.0)
            marks[:, j * DH : (j + 1) * DH] = mark.astype(jnp.bfloat16)
        for copy in scalars:
            copy.wait()
        shape = (rows, DH)
        row = lax.broadcasted_iota(jnp.int32, shape, 0)
        spot = lax.rem(lax.broadcasted_iota(jnp.int32, shape, 1), positions)
        table = jnp.full(shape, NEG, jnp.float32)
        for b in range(rows):
            live = (row == b) & (spot < lengths[b] - me * positions)
            table = jnp.where(live, 0.0, table)
        bias[...] = table
        shape = (rows, extent)
        row = lax.broadcasted_iota(jnp.int32, shape, 0)
        lane = lax.broadcasted_iota(jnp.int32, shape, 1)
        table = jnp.zeros(shape, jnp.float32)
        for b in range(rows):
            for e in range(entries):
                here = (row == b) & (lane >= e * tokens) & (lane < (e + 1) * tokens)
                for j in range(ids.shape[0]):
                    match = here & (jnp.full(shape, ids[j, b], jnp.int32) == me * entries + e)
                    table = jnp.where(match, table + 1.0, table)
        ccounts[...] = table
        cbias[...] = jnp.where(table > 0.0, 0.0, NEG)

    def quads_of(source, turn, slot):
        block = source[:, lanes_of(owner(turn, slot))].astype(jnp.float32)
        found = []
        for pair in range(pairs):
            first = block[:, 2 * pair * DH : (2 * pair + 1) * DH]
            second = block[:, (2 * pair + 1) * DH : (2 * pair + 2) * DH]
            quad = jnp.concatenate(
                [
                    jnp.concatenate([first, zero], axis=1),
                    jnp.concatenate([zero, second], axis=1),
                ],
                axis=0,
            )
            found.append(quad.astype(jnp.bfloat16))
        return found

    def piece_of(pair):
        return slice(pair * 2 * DH, (pair + 1) * 2 * DH)

    def score(turn):
        blank = jnp.zeros((pair_rows, 2 * DH), jnp.bfloat16)
        found = None
        for s in range(gather):
            for pair, quad in enumerate(quads_of(squery, turn, s)):
                at = s * pairs + pair
                query = jnp.concatenate(
                    [quad if i == at else blank for i in range(gather * pairs)], axis=0
                )
                held = keys[turn, s, :, :, piece_of(pair)].reshape(rows * positions, 2 * DH)
                part = lax.dot_general(
                    held, query, (((1,), (1,)), ((), ())), preferred_element_type=jnp.float32
                )
                found = part if found is None else found + part
        column = lax.rem(lax.broadcasted_iota(jnp.int32, (positions, total), 1), rows)
        folded = found[:positions]
        for b in range(1, rows):
            folded = jnp.where(column == b, found[b * positions : (b + 1) * positions], folded)
        folded = jnp.concatenate([folded] * copies, axis=0)
        scores[turn % 2] = folded.T

    def cross_score(turn):
        for s in range(gather):
            for pair, quad in enumerate(quads_of(cquery, turn, s)):
                at = s * pairs + pair
                held = dkeys[turn, s, :, :, piece_of(pair)].reshape(extent, 2 * DH)
                cscores[turn % 2, at * pair_rows : (at + 1) * pair_rows] = lax.dot_general(
                    quad,
                    held,
                    (((1,), (1,)), ((), ())),
                    preferred_element_type=jnp.float32,
                )

    def weigh(found, table, number, share):
        depth = found.shape[1]
        level = found.reshape(total // rows, rows, depth) * (DH ** (-0.5)) + table[None]
        peak = jnp.maximum(jnp.max(level, axis=2, keepdims=True), FLOOR)
        weights = jnp.exp(level - peak)
        if number is not None:
            weights = weights * number[None]
        den = jnp.maximum(jnp.sum(weights, axis=2, keepdims=True) * share, 0.5)
        inverse, level = 1.0 / den, peak + jnp.log(den)
        return (
            weights.reshape(total, depth).astype(jnp.bfloat16),
            inverse.reshape(total, 1),
            level.reshape(total, 1),
        )

    def weigh_both(turn):
        return (
            weigh(scores[turn % 2], bias[...], None, 1.0 / copies),
            weigh(cscores[turn % 2], cbias[...], ccounts[...], 1.0),
        )

    def combine(turn, slots, found):
        (weights, inverse, level), (cweights, cinverse, clevel) = found
        for s in slots:
            tile = jnp.zeros((pair_rows, DH), jnp.float32)
            for pair in range(pairs):
                at = (s * pairs + pair) * pair_rows
                mine = slice(at, at + pair_rows)
                expanded = jnp.concatenate([weights[mine]] * chunks, axis=1) * marks[...]
                acc = jnp.dot(
                    expanded,
                    values[turn, s, :, :, piece_of(pair)].reshape(rows * positions, 2 * DH),
                    preferred_element_type=jnp.float32,
                )
                cacc = jnp.dot(
                    cweights[mine],
                    dvalues[turn, s, :, :, piece_of(pair)].reshape(extent, 2 * DH),
                    preferred_element_type=jnp.float32,
                )
                for h in range(2):
                    these = slice(h * rows, (h + 1) * rows)
                    rest = slice(h * DH, (h + 1) * DH)
                    at_head = slice(at + h * rows, at + (h + 1) * rows)
                    part = jnp.concatenate(
                        [
                            acc[these, rest] * inverse[at_head],
                            cacc[these, rest] * cinverse[at_head],
                        ],
                        axis=0,
                    )
                    head = 2 * pair + h
                    outbox[turn, s, :, head * DH : (head + 1) * DH] = part.astype(jnp.bfloat16)
                    both = jnp.concatenate([level[at_head], clevel[at_head]], axis=0)
                    tile = jnp.where(lax.rem(tag, heads) == head, both, tile)
            outbox[turn, s, :, span:] = packed(tile)

    def spread(tile, head):
        return jnp.broadcast_to(tile[:, head : head + 1], (pair_rows, DH))

    def level_of(box):
        raw = box[:, span:].astype(jnp.float32)
        full = raw + pltpu.roll(raw, DH - heads, 1) + pltpu.roll(raw, DH - 2 * heads, 1)
        return jnp.where(tag < heads, full, NEG)

    def packed(level):
        high = level.astype(jnp.bfloat16).astype(jnp.float32)
        rest = level - high
        middle = rest.astype(jnp.bfloat16).astype(jnp.float32)
        low = rest - middle
        level = jnp.where(tag < heads, high, jnp.where(tag < 2 * heads, middle, low))
        return level.astype(jnp.bfloat16)

    def kept(turn, place):
        return outbox.at[turn, 2 * place + 1]

    def merge(turn, place):
        step = turn * members + place
        mine, other_box = kept(turn, place), sidebox.at[step]
        first, second = level_of(mine), level_of(other_box)
        top = jnp.maximum(first, second)
        share, other = jnp.exp(first - top), jnp.exp(second - top)
        both = share + other
        inverse = 1.0 / both
        share, other = share * inverse, other * inverse
        for h in range(heads):
            piece = slice(h * DH, (h + 1) * DH)
            part = mine[:, piece].astype(jnp.float32) * spread(share, h)
            part = part + other_box[:, piece].astype(jnp.float32) * spread(other, h)
            merged[step, :, piece] = part.astype(jnp.bfloat16)
        level = top + jnp.log(both)
        level = jnp.where(tag < heads, level, 0.0)
        level = (
            level
            + jnp.where(tag < 2 * heads, pltpu.roll(level, heads, 1), 0.0)
            + pltpu.roll(level, 2 * heads, 1)
        )
        merged[step, :, span:] = packed(level)

    def arrive(name):
        turn = int(name[1])
        slots = everything if len(name) == 2 else (2 * int(name[2]), 2 * int(name[2]) + 1)
        for kind in (0, 2) if name[0] == "K" else (1, 3):
            for copy in stream(kind, turn, slots):
                copy.wait()

    held = {}

    def run(action):
        name, turn = action[0], int(action[1:2] or 0)
        places = [int(action[2])] if len(action) > 2 else range(members)
        if name == "Q":
            small[turn].wait()
        if name == "M":
            prepare()
        if name in "KV":
            arrive(action)
        if name == "+":
            launch(turn)
        if name == "S":
            score(turn)
            cross_score(turn)
        if name == "W":
            held[turn] = weigh_both(turn)
        if name == "C":
            if turn not in held:
                held[turn] = weigh_both(turn)
            combine(turn, [2 * p + c for p in places for c in range(2)], held[turn])
        if name == "B":
            pl.semaphore_wait(barrier, chips)
        if name == "H":
            for place in places:
                handover(turn, place).start()
        if name == "P":
            for place in places:
                if (turn, place) != steps[-1]:
                    handover(turn, place).wait_recv()
                    merge(turn, place)
                    message(turn, place).start()

    for action in plan:
        run(action)

    small[2].wait()
    small[3].wait()
    query_own = squery[:, own].astype(jnp.float32)
    product = query_own * nkey[...].astype(jnp.float32)
    level_own = jnp.full((rows, DH), NEG, jnp.float32)
    short = tag[:rows]
    for h in range(heads):
        value = jnp.sum(product[:, h * DH : (h + 1) * DH], axis=1, keepdims=True) * (DH ** (-0.5))
        level_own = jnp.where(short == h, value, level_own)
    level_own = jnp.concatenate([level_own, jnp.full((rows, DH), NEG, jnp.float32)], axis=0)

    last = steps[-1]
    boxes = [(kept(*last), None)]
    boxes += [(inbox.at[k], message(*step)) for k, step in enumerate(steps[:-1])]
    boxes.insert(len(boxes) - 1, (sidebox.at[len(steps) - 1], handover(*last)))
    top = level_own
    for k, (box, copy) in enumerate(boxes):
        if copy is not None:
            copy.wait_recv()
        level = level_of(box)
        stats[k] = level
        top = jnp.maximum(top, level)
    share = jnp.exp(level_own - top)
    both = share
    sums = [
        jnp.concatenate([nvalue[:, h * DH : (h + 1) * DH].astype(jnp.float32), zero], axis=0)
        * spread(share, h)
        for h in range(heads)
    ]
    for k, (box, _) in enumerate(boxes):
        share = jnp.exp(stats[k] - top)
        both = both + share
        for h in range(heads):
            part = box[:, h * DH : (h + 1) * DH].astype(jnp.float32)
            sums[h] = sums[h] + part * spread(share, h)
    inverse = 1.0 / both
    for h in range(heads):
        result = sums[h] * spread(inverse, h)
        out[:, h * DH : (h + 1) * DH] = result.astype(jnp.bfloat16)

    for step in steps[:-1]:
        message(*step).wait_send()
    for step in steps:
        handover(*step).wait_send()


def on_device(
    self_query,
    new_key,
    new_value,
    cache_keys,
    cache_values,
    lengths,
    db_keys,
    db_values,
    cross_query,
    neighbour_ids,
):
    parts = lax.axis_size("seq")
    rows, positions, width = cache_keys.shape
    entries, tokens, _ = db_keys.shape
    span = width // parts
    chips = parts // 2
    gather = min(parts, DH * DH // (span * rows))
    groups = parts // gather
    total = gather * span // DH * rows
    half = jnp.bfloat16
    anywhere = pl.BlockSpec(memory_space=pl.ANY)
    vmem = pl.BlockSpec(memory_space=pltpu.VMEM)
    box = (2 * rows, span + DH)
    out = pl.pallas_call(
        functools.partial(kernel, parts, gather, ['K0', 'V0', 'K1', 'V1', 'K2', 'V2', 'K3', 'V30', 'V31'], 4, ['Q0', 'K0', '+2', 'Q1', 'S0', 'V0', '+2', 'M', 'C0', 'K1', '+9', '+9', 'S1', 'B', 'H0', 'V1', 'K2', 'S2', 'C1', 'P0', 'H1', 'V2', 'K3', 'S3', 'C2', 'P1', 'H2', 'V30', 'C30', 'H30', 'P2', 'V31', 'C31', 'H31', 'P30']),
        out_shape=pltpu.VMEM((2 * rows, span), half),
        in_specs=[anywhere] * 10,
        out_specs=vmem,
        scratch_shapes=[
            pltpu.SMEM(lengths.shape, jnp.int32),
            pltpu.SMEM(neighbour_ids.shape[::-1], jnp.int32),
            pltpu.VMEM((groups, gather, rows, positions, span), half),
            pltpu.VMEM((groups, gather, rows, positions, span), half),
            pltpu.VMEM((groups, gather, entries, tokens, span), half),
            pltpu.VMEM((groups, gather, entries, tokens, span), half),
            pltpu.VMEM((rows, width), half),
            pltpu.VMEM((rows, width), half),
            pltpu.VMEM((rows, span), half),
            pltpu.VMEM((rows, span), half),
            pltpu.VMEM((2 * rows, rows * positions), half),
            pltpu.VMEM((rows, DH), jnp.float32),
            pltpu.VMEM((rows, entries * tokens), jnp.float32),
            pltpu.VMEM((rows, entries * tokens), jnp.float32),
            pltpu.VMEM((2, total, DH), jnp.float32),
            pltpu.VMEM((2, total, entries * tokens), jnp.float32),
            pltpu.VMEM((groups, gather, *box), half),
            pltpu.VMEM((chips, *box), half),
            pltpu.VMEM((chips, *box), half),
            pltpu.VMEM((chips, *box), half),
            pltpu.VMEM((chips + 1, 2 * rows, DH), jnp.float32),
            pltpu.SemaphoreType.DMA((4, groups, gather)),
            pltpu.SemaphoreType.DMA((6,)),
            pltpu.SemaphoreType.DMA((chips,)),
            pltpu.SemaphoreType.DMA((chips,)),
            pltpu.SemaphoreType.DMA((chips,)),
            pltpu.SemaphoreType.DMA((chips,)),
        ],
        compiler_params=pltpu.CompilerParams(
            collective_id=0, has_side_effects=True, vmem_limit_bytes=48 * 1024 * 1024
        ),
    )(
        *[
            pltpu.with_memory_space_constraint(array, pltpu.HBM)
            for array in (
                lengths,
                neighbour_ids.T,
                self_query,
                new_key,
                new_value,
                cache_keys,
                cache_values,
                db_keys,
                db_values,
                cross_query,
            )
        ]
    )
    return out[:rows], out[rows:]


def solution(mesh):
    in_specs = (
        P("groups", None),
        P("groups", None),
        P("groups", None),
        P("groups", "seq", None),
        P("groups", "seq", None),
        P("groups"),
        P(("groups", "seq"), None, None),
        P(("groups", "seq"), None, None),
        P("groups", None),
        P("groups", None),
    )
    out_specs = (P("groups", "seq"), P("groups", "seq"))
    return jax.shard_map(
        on_device, mesh=mesh, in_specs=in_specs, out_specs=out_specs, check_vma=False
    )
```

```python
import functools

import jax
import jax.numpy as jnp
from jax import lax
from jax.experimental import pallas as pl
from jax.experimental.pallas import tpu as pltpu
from jax.sharding import PartitionSpec as P

DH = 128
NEG = -1e30
FLOOR = -1e29
MESH = pl.DeviceIdType.MESH


def mirrored(index, flip, count):
    if count & (count - 1):
        return lax.rem(index + flip, count)
    result, bit = 0, 1
    while bit < count:
        digit = lax.rem(index // bit, 2)
        result = result + bit * (1 - digit if flip & bit else digit)
        bit *= 2
    return result


def kernel(
    parts,
    gather,
    loads,
    ahead,
    plan,
    lengths_in,
    ids_in,
    self_query,
    new_key,
    new_value,
    cache_keys,
    cache_values,
    db_keys,
    db_values,
    cross_query,
    out,
    lengths,
    ids,
    keys,
    values,
    dkeys,
    dvalues,
    squery,
    cquery,
    nkey,
    nvalue,
    marks,
    bias,
    cbias,
    ccounts,
    scores,
    cscores,
    outbox,
    sidebox,
    merged,
    inbox,
    stream_sem,
    small_sem,
    send_sem,
    recv_sem,
    side_send,
    side_recv,
):
    me = lax.axis_index("seq")
    rows, positions, width = cache_keys.shape
    entries, tokens, _ = db_keys.shape
    extent = entries * tokens
    span = width // parts
    heads = span // DH
    pairs = heads // 2
    pair_rows = 2 * rows
    groups = parts // gather
    members = gather // 2
    chips = parts // 2
    total = gather * heads * rows
    copies = DH // positions
    chunks = rows // copies

    core = lax.rem(me, 2)
    chip = me // 2
    partner = chip * 2 + 1 - core
    member = lax.rem(chip, members)
    group = chip // members

    def group_at(turn):
        return mirrored(group, groups - 1 - turn, groups)

    def member_at(place):
        return lax.rem(member + 1 + place, members)

    def peer(turn, place):
        return (group_at(turn) * members + member_at(place)) * 2 + core

    def lanes_of(device):
        return pl.ds(pl.multiple_of(device * span, span), span)

    def owner(turn, slot):
        return peer(turn, slot // 2) - core + (core if slot % 2 else 1 - core)

    def stream(kind, turn, slots):
        source, dest = (
            (cache_keys, keys),
            (cache_values, values),
            (db_keys, dkeys),
            (db_values, dvalues),
        )[kind]
        return [
            pltpu.make_async_copy(
                source.at[:, :, lanes_of(owner(turn, s))],
                dest.at[turn, s],
                stream_sem.at[kind, turn, s],
            )
            for s in slots
        ]

    def handover(turn, place):
        step = turn * members + place
        return pltpu.make_async_remote_copy(
            src_ref=outbox.at[turn, 2 * place],
            dst_ref=sidebox.at[step],
            send_sem=side_send.at[step],
            recv_sem=side_recv.at[step],
            device_id={"seq": partner},
            device_id_type=MESH,
        )

    def message(turn, place):
        step = turn * members + place
        return pltpu.make_async_remote_copy(
            src_ref=merged.at[step],
            dst_ref=inbox.at[step],
            send_sem=send_sem.at[step],
            recv_sem=recv_sem.at[step],
            device_id={"seq": peer(turn, place)},
            device_id_type=MESH,
        )

    steps = [(turn, place) for turn in range(groups) for place in range(members)]

    own = lanes_of(me)
    small = [
        pltpu.make_async_copy(self_query, squery, small_sem.at[0]),
        pltpu.make_async_copy(cross_query, cquery, small_sem.at[1]),
        pltpu.make_async_copy(new_key.at[:, own], nkey, small_sem.at[2]),
        pltpu.make_async_copy(new_value.at[:, own], nvalue, small_sem.at[3]),
    ]
    scalars = [
        pltpu.make_async_copy(lengths_in, lengths, small_sem.at[4]),
        pltpu.make_async_copy(ids_in, ids, small_sem.at[5]),
    ]
    everything = range(gather)
    queue = []
    for name in loads:
        turn = int(name[1])
        slots = everything if len(name) == 2 else (2 * int(name[2]), 2 * int(name[2]) + 1)
        for kind in (0, 2) if name[0] == "K" else (1, 3):
            queue.append((kind, turn, slots))

    def launch(count):
        for _ in range(count):
            if queue:
                for copy in stream(*queue.pop(0)):
                    copy.start()

    small[0].start()
    small[1].start()
    launch(2)
    barrier = pltpu.get_barrier_semaphore()
    for turn, place in steps[:-1]:
        pl.semaphore_signal(
            barrier, inc=1, device_id={"seq": peer(turn, place)}, device_id_type=MESH
        )
    pl.semaphore_signal(barrier, inc=1, device_id={"seq": partner}, device_id_type=MESH)

    for copy in scalars:
        copy.start()
    launch(ahead)
    small[2].start()
    small[3].start()
    tag = lax.broadcasted_iota(jnp.int32, (pair_rows, DH), 1)
    zero = jnp.zeros((rows, DH), jnp.float32)

    def prepare():
        line = lax.rem(lax.broadcasted_iota(jnp.int32, (pair_rows, DH), 0), rows)
        for j in range(chunks):
            mark = jnp.where(line == j * copies + tag // positions, 1.0, 0.0)
            marks[:, j * DH : (j + 1) * DH] = mark.astype(jnp.bfloat16)
        for copy in scalars:
            copy.wait()
        shape = (rows, DH)
        row = lax.broadcasted_iota(jnp.int32, shape, 0)
        spot = lax.rem(lax.broadcasted_iota(jnp.int32, shape, 1), positions)
        table = jnp.full(shape, NEG, jnp.float32)
        for b in range(rows):
            live = (row == b) & (spot < lengths[b] - me * positions)
            table = jnp.where(live, 0.0, table)
        bias[...] = table
        shape = (rows, extent)
        row = lax.broadcasted_iota(jnp.int32, shape, 0)
        lane = lax.broadcasted_iota(jnp.int32, shape, 1)
        table = jnp.zeros(shape, jnp.float32)
        for b in range(rows):
            for e in range(entries):
                here = (row == b) & (lane >= e * tokens) & (lane < (e + 1) * tokens)
                for j in range(ids.shape[0]):
                    match = here & (jnp.full(shape, ids[j, b], jnp.int32) == me * entries + e)
                    table = jnp.where(match, table + 1.0, table)
        ccounts[...] = table
        cbias[...] = jnp.where(table > 0.0, 0.0, NEG)

    def quads_of(source, turn, slot):
        block = source[:, lanes_of(owner(turn, slot))].astype(jnp.float32)
        found = []
        for pair in range(pairs):
            first = block[:, 2 * pair * DH : (2 * pair + 1) * DH]
            second = block[:, (2 * pair + 1) * DH : (2 * pair + 2) * DH]
            quad = jnp.concatenate(
                [
                    jnp.concatenate([first, zero], axis=1),
                    jnp.concatenate([zero, second], axis=1),
                ],
                axis=0,
            )
            found.append(quad.astype(jnp.bfloat16))
        return found

    def piece_of(pair):
        return slice(pair * 2 * DH, (pair + 1) * 2 * DH)

    def score(turn, staged=False):
        blank = jnp.zeros((pair_rows, 2 * DH), jnp.bfloat16)
        found = None
        for s in range(gather):
            if staged:
                stream(0, turn, [s])[0].wait()
            for pair, quad in enumerate(quads_of(squery, turn, s)):
                at = s * pairs + pair
                query = jnp.concatenate(
                    [quad if i == at else blank for i in range(gather * pairs)], axis=0
                )
                held = keys[turn, s, :, :, piece_of(pair)].reshape(rows * positions, 2 * DH)
                part = lax.dot_general(
                    held, query, (((1,), (1,)), ((), ())), preferred_element_type=jnp.float32
                )
                found = part if found is None else found + part
        column = lax.rem(lax.broadcasted_iota(jnp.int32, (positions, total), 1), rows)
        folded = found[:positions]
        for b in range(1, rows):
            folded = jnp.where(column == b, found[b * positions : (b + 1) * positions], folded)
        folded = jnp.concatenate([folded] * copies, axis=0)
        scores[turn % 2] = folded.T

    def cross_score(turn):
        count = gather * pairs
        batch = min(4, count)
        blank = jnp.zeros((pair_rows, 2 * DH), jnp.bfloat16)
        quads = sum((quads_of(cquery, turn, s) for s in range(gather)), [])
        for start in range(0, count, batch):
            found = None
            for at in range(start, start + batch):
                query = jnp.concatenate(
                    [quads[at] if i == at else blank for i in range(start, start + batch)], axis=0
                )
                held = dkeys[turn, at // pairs, :, :, piece_of(at % pairs)]
                part = lax.dot_general(
                    held.reshape(extent, 2 * DH),
                    query,
                    (((1,), (1,)), ((), ())),
                    preferred_element_type=jnp.float32,
                )
                found = part if found is None else found + part
            cscores[turn % 2, start * pair_rows : (start + batch) * pair_rows] = found.T

    def weigh(found, table, number, share):
        depth = found.shape[1]
        level = found.reshape(total // rows, rows, depth) * (DH ** (-0.5)) + table[None]
        peak = jnp.maximum(jnp.max(level, axis=2, keepdims=True), FLOOR)
        weights = jnp.exp(level - peak)
        if number is not None:
            weights = weights * number[None]
        den = jnp.maximum(jnp.sum(weights, axis=2, keepdims=True) * share, 0.5)
        inverse, level = 1.0 / den, peak + jnp.log(den)
        return (
            weights.reshape(total, depth).astype(jnp.bfloat16),
            inverse.reshape(total, 1),
            level.reshape(total, 1),
        )

    def weigh_both(turn):
        return (
            weigh(scores[turn % 2], bias[...], None, 1.0 / copies),
            weigh(cscores[turn % 2], cbias[...], ccounts[...], 1.0),
        )

    def combine(turn, slots, found):
        (weights, inverse, level), (cweights, cinverse, clevel) = found
        for s in slots:
            tile = jnp.zeros((pair_rows, DH), jnp.float32)
            for pair in range(pairs):
                at = (s * pairs + pair) * pair_rows
                mine = slice(at, at + pair_rows)
                expanded = jnp.concatenate([weights[mine]] * chunks, axis=1) * marks[...]
                acc = jnp.dot(
                    expanded,
                    values[turn, s, :, :, piece_of(pair)].reshape(rows * positions, 2 * DH),
                    preferred_element_type=jnp.float32,
                )
                cacc = jnp.dot(
                    cweights[mine],
                    dvalues[turn, s, :, :, piece_of(pair)].reshape(extent, 2 * DH),
                    preferred_element_type=jnp.float32,
                )
                for h in range(2):
                    these = slice(h * rows, (h + 1) * rows)
                    rest = slice(h * DH, (h + 1) * DH)
                    at_head = slice(at + h * rows, at + (h + 1) * rows)
                    part = jnp.concatenate(
                        [
                            acc[these, rest] * inverse[at_head],
                            cacc[these, rest] * cinverse[at_head],
                        ],
                        axis=0,
                    )
                    head = 2 * pair + h
                    outbox[turn, s, :, head * DH : (head + 1) * DH] = part.astype(jnp.bfloat16)
                    both = jnp.concatenate([level[at_head], clevel[at_head]], axis=0)
                    tile = jnp.where(lax.rem(tag, heads) == head, both, tile)
            outbox[turn, s, :, span:] = packed(tile)

    def spread(tile, head):
        return jnp.broadcast_to(tile[:, head : head + 1], (pair_rows, DH))

    def level_of(box):
        raw = box[:, span:].astype(jnp.float32)
        full = raw + pltpu.roll(raw, DH - heads, 1) + pltpu.roll(raw, DH - 2 * heads, 1)
        return jnp.where(tag < heads, full, NEG)

    def packed(level):
        high = level.astype(jnp.bfloat16).astype(jnp.float32)
        rest = level - high
        middle = rest.astype(jnp.bfloat16).astype(jnp.float32)
        low = rest - middle
        level = jnp.where(tag < heads, high, jnp.where(tag < 2 * heads, middle, low))
        return level.astype(jnp.bfloat16)

    def kept(turn, place):
        return outbox.at[turn, 2 * place + 1]

    def merge(turn, place):
        step = turn * members + place
        mine, other_box = kept(turn, place), sidebox.at[step]
        first, second = level_of(mine), level_of(other_box)
        top = jnp.maximum(first, second)
        share, other = jnp.exp(first - top), jnp.exp(second - top)
        both = share + other
        inverse = 1.0 / both
        share, other = share * inverse, other * inverse
        for h in range(heads):
            piece = slice(h * DH, (h + 1) * DH)
            part = mine[:, piece].astype(jnp.float32) * spread(share, h)
            part = part + other_box[:, piece].astype(jnp.float32) * spread(other, h)
            merged[step, :, piece] = part.astype(jnp.bfloat16)
        level = top + jnp.log(both)
        level = jnp.where(tag < heads, level, 0.0)
        level = (
            level
            + jnp.where(tag < 2 * heads, pltpu.roll(level, heads, 1), 0.0)
            + pltpu.roll(level, 2 * heads, 1)
        )
        merged[step, :, span:] = packed(level)

    def arrive(name):
        turn = int(name[1])
        slots = everything if len(name) == 2 else (2 * int(name[2]), 2 * int(name[2]) + 1)
        for kind in (0, 2) if name[0] == "K" else (1, 3):
            for copy in stream(kind, turn, slots):
                copy.wait()

    held = {}

    def run(action):
        name, turn = action[0], int(action[1:2] or 0)
        places = [int(action[2])] if len(action) > 2 else range(members)
        if name == "Q":
            small[turn].wait()
        if name == "M":
            prepare()
        if name in "KV":
            arrive(action)
        if name == "+":
            launch(turn)
        if name == "Z":
            score(turn, True)
            cross_score(turn)
        if name == "S":
            score(turn)
            cross_score(turn)
        if name == "W":
            held[turn] = weigh_both(turn)
        if name == "C":
            if turn not in held:
                held[turn] = weigh_both(turn)
            combine(turn, [2 * p + c for p in places for c in range(2)], held[turn])
        if name == "B":
            pl.semaphore_wait(barrier, chips)
        if name == "H":
            for place in places:
                handover(turn, place).start()
        if name == "P":
            outgoing = [place for place in places if (turn, place) != steps[-1]]
            for place in outgoing:
                handover(turn, place).wait_recv()
            for place in outgoing:
                merge(turn, place)
            for place in outgoing:
                message(turn, place).start()

    for action in plan:
        run(action)

    small[2].wait()
    small[3].wait()
    query_own = squery[:, own].astype(jnp.float32)
    product = query_own * nkey[...].astype(jnp.float32)
    level_own = jnp.full((rows, DH), NEG, jnp.float32)
    short = tag[:rows]
    for h in range(heads):
        value = jnp.sum(product[:, h * DH : (h + 1) * DH], axis=1, keepdims=True) * (DH ** (-0.5))
        level_own = jnp.where(short == h, value, level_own)
    level_own = jnp.concatenate([level_own, jnp.full((rows, DH), NEG, jnp.float32)], axis=0)

    last = steps[-1]
    waves = [
        [(kept(*last), None), (sidebox.at[len(steps) - 1], handover(*last))],
        [(inbox.at[k], message(*step)) for k, step in enumerate(steps[:-1])],
    ]

    def fold(top, both, sums, boxes):
        for _, copy in boxes:
            if copy is not None:
                copy.wait_recv()
        levels = [level_of(box) for box, _ in boxes]
        peak = functools.reduce(jnp.maximum, levels, top)
        shares = [jnp.exp(level - peak) for level in levels]
        scale = both * jnp.exp(top - peak)
        both = functools.reduce(jnp.add, shares, scale)
        inverse = 1.0 / both
        shares = [share * inverse for share in shares]
        scale = scale * inverse
        for h in range(heads):
            result = sums[h] * spread(scale, h)
            for share, (box, _) in zip(shares, boxes):
                part = box[:, h * DH : (h + 1) * DH].astype(jnp.float32)
                result = result + part * spread(share, h)
            sums[h] = result
        return peak, both, sums

    sums = [
        jnp.concatenate([nvalue[:, h * DH : (h + 1) * DH].astype(jnp.float32), zero], axis=0)
        for h in range(heads)
    ]
    top, both = level_own, jnp.ones((pair_rows, DH), jnp.float32)
    for wave in waves:
        top, both, sums = fold(top, both, sums, wave)
    for h in range(heads):
        out[:, h * DH : (h + 1) * DH] = sums[h].astype(jnp.bfloat16)

    for step in steps[:-1]:
        message(*step).wait_send()
    for step in steps:
        handover(*step).wait_send()


def on_device(
    self_query,
    new_key,
    new_value,
    cache_keys,
    cache_values,
    lengths,
    db_keys,
    db_values,
    cross_query,
    neighbour_ids,
):
    parts = lax.axis_size("seq")
    rows, positions, width = cache_keys.shape
    entries, tokens, _ = db_keys.shape
    span = width // parts
    chips = parts // 2
    gather = min(parts, DH * DH // (span * rows))
    groups = parts // gather
    total = gather * span // DH * rows
    half = jnp.bfloat16
    anywhere = pl.BlockSpec(memory_space=pl.ANY)
    vmem = pl.BlockSpec(memory_space=pltpu.VMEM)
    box = (2 * rows, span + DH)
    out = pl.pallas_call(
        functools.partial(kernel, parts, gather, ['K0', 'K1', 'V0', 'K2', 'V1', 'K3', 'V2', 'V30', 'V31'], 8, ['Q0', 'K0', '+2', 'Q1', 'M', 'S0', 'K1', 'V0', '+9', '+9', 'S1', 'C0', 'B', 'H0', 'V1', 'K2', 'S2', 'C1', 'P0', 'H1', 'V2', 'K3', 'S3', 'C2', 'P1', 'H2', 'V30', 'C30', 'H30', 'P2', 'V31', 'C31', 'H31', 'P30']),
        out_shape=pltpu.VMEM((2 * rows, span), half),
        in_specs=[anywhere] * 10,
        out_specs=vmem,
        scratch_shapes=[
            pltpu.SMEM(lengths.shape, jnp.int32),
            pltpu.SMEM(neighbour_ids.shape[::-1], jnp.int32),
            pltpu.VMEM((groups, gather, rows, positions, span), half),
            pltpu.VMEM((groups, gather, rows, positions, span), half),
            pltpu.VMEM((groups, gather, entries, tokens, span), half),
            pltpu.VMEM((groups, gather, entries, tokens, span), half),
            pltpu.VMEM((rows, width), half),
            pltpu.VMEM((rows, width), half),
            pltpu.VMEM((rows, span), half),
            pltpu.VMEM((rows, span), half),
            pltpu.VMEM((2 * rows, rows * positions), half),
            pltpu.VMEM((rows, DH), jnp.float32),
            pltpu.VMEM((rows, entries * tokens), jnp.float32),
            pltpu.VMEM((rows, entries * tokens), jnp.float32),
            pltpu.VMEM((2, total, DH), jnp.float32),
            pltpu.VMEM((2, total, entries * tokens), jnp.float32),
            pltpu.VMEM((groups, gather, *box), half),
            pltpu.VMEM((chips, *box), half),
            pltpu.VMEM((chips, *box), half),
            pltpu.VMEM((chips, *box), half),
            pltpu.SemaphoreType.DMA((4, groups, gather)),
            pltpu.SemaphoreType.DMA((6,)),
            pltpu.SemaphoreType.DMA((chips,)),
            pltpu.SemaphoreType.DMA((chips,)),
            pltpu.SemaphoreType.DMA((chips,)),
            pltpu.SemaphoreType.DMA((chips,)),
        ],
        compiler_params=pltpu.CompilerParams(
            collective_id=0, has_side_effects=True, vmem_limit_bytes=48 * 1024 * 1024
        ),
    )(
        *[
            pltpu.with_memory_space_constraint(array, pltpu.HBM)
            for array in (
                lengths,
                neighbour_ids.T,
                self_query,
                new_key,
                new_value,
                cache_keys,
                cache_values,
                db_keys,
                db_values,
                cross_query,
            )
        ]
    )
    return out[:rows], out[rows:]


def solution(mesh):
    in_specs = (
        P("groups", None),
        P("groups", None),
        P("groups", None),
        P("groups", "seq", None),
        P("groups", "seq", None),
        P("groups"),
        P(("groups", "seq"), None, None),
        P(("groups", "seq"), None, None),
        P("groups", None),
        P("groups", None),
    )
    out_specs = (P("groups", "seq"), P("groups", "seq"))
    return jax.shard_map(
        on_device, mesh=mesh, in_specs=in_specs, out_specs=out_specs, check_vma=False
    )
```
